256 devices in a mesh: row: 16 (over y, x), col: 16 (over z, core).
Axes of the slice: x: 4, y: 4, z: 8, core: 2. Of those that a mesh axis runs over, the one named last changes fastest.
Arguments:
- tokens: bfloat16 [1024, 7168], P('col', 'row'), may hold values from -6 to 6
- routes: int32 [1024, 8], P('col'), may hold values from 0 to 31, all different within a row; in each aligned block of 64 rows (0 to 63, 64 to 127, ...) at most 40 rows name the same one
- gates: float32 [1024, 8], P('col'), may hold values from 0.05 to 0.5
- w_gate: bfloat16 [32, 7168, 2048], P('col', None, 'row'), may hold values from -0.0625 to 0.0625
- w_up: bfloat16 [32, 7168, 2048], P('col', None, 'row'), may hold values from -0.0625 to 0.0625
- w_down: bfloat16 [32, 2048, 7168], P('col', 'row'), may hold values from -0.125 to 0.125
Outputs:
- mixed: bfloat16 [1024, 7168], P('col', 'row')
The draws below stay inside these ranges and needn't reach their ends.
Inputs may be any that keep to these rules, and one draw needn't show every extreme that they name: `routes`: the 8 experts of a token are distinct. Among the 64 tokens of one index of col (aligned blocks of 64 tokens), no expert is chosen more than 40 times, and some expert is chosen exactly 40 times.
All inputs are finite; a program needn't handle non-finite values.
Results may differ from the reference program's by a relative error of at most 0.015.
Values may be sent and summed in bfloat16 or wider, within the bound.
No kernel may reach another device: no remote copies, remote signals or barrier semaphores. Data moves between devices by JAX's collectives and lax.ppermute only.
A program may use at most 128 MiB of HBM per device.

```python
import math
import jax
import jax.numpy as jnp
import numpy as np
from jax import lax

D = 7168
FF = 2048
TOP = 8
TOK_DEV = 64
CAP = 40
EXPERTS = 32
TOKENS = 1024
SLOTS = 640
FF_BLOCK = 128
N_ROW = 16
N_COL = 16


def steps_of(rng, shape, cuts, least, high):
    def one(dim, parts):
        steps = jax.random.uniform(jax.random.fold_in(jax.random.fold_in(rng, 6), dim), (parts,), jnp.float32, least / len(cuts), high / len(cuts))
        return jnp.repeat(jnp.exp(steps), shape[dim] // parts).reshape((-1,) + (1,) * (len(shape) - dim - 1))

    factor_of = one(*cuts[0])
    for cut in cuts[1:]:
        factor_of = factor_of * one(*cut)
    return factor_of


def deal_out(rng, own, number, rows, count, top, most, lean):
    sequence = jax.random.permutation(rng, count)
    packed, usual = portions_of(count, rows * top, most, lean, True), portions_of(count, rows * top, most, lean, False)
    places = jnp.arange(count)

    def named(lengths, turn):
        used = int((lengths > 0).sum())
        fixed = max(1, used // 4)
        moved = fixed + (places - fixed + turn * (used - fixed)) % max(1, count - fixed)
        return jnp.zeros((count,), jnp.int32).at[sequence[jnp.where(places < fixed, places, moved)]].set(jnp.asarray(lengths, jnp.int32))

    lengths = jnp.where(number % 4 == 0, named(packed, number // 4), named(usual, number - number // 4 - 1))
    mixed = jax.random.permutation(jax.random.fold_in(own, 3), count)
    donor, taker = mixed[0:count // 2 * 2:2], mixed[1:count // 2 * 2:2]
    margin = jnp.minimum(lengths[donor] - 1, most - lengths[taker]) // 2
    margin = jnp.where((donor == sequence[0]) | (taker == sequence[0]) | (lengths[taker] == 0), 0, jnp.maximum(margin, 0))
    moved = jax.random.randint(jax.random.fold_in(own, 4), (count // 2,), 0, 1 << 20) % (margin + 1)
    lengths = lengths.at[donor].add(-moved).at[taker].add(moved)
    members = jnp.searchsorted(jnp.cumsum(lengths), jnp.arange(rows * top), side="right").astype(jnp.int32)
    grid = members.reshape(top, rows).T
    grid = grid[jax.random.permutation(jax.random.fold_in(own, 1), rows)]
    turn = jax.random.randint(jax.random.fold_in(own, 2), (rows, 1), 0, top)
    return jnp.take_along_axis(grid, (jnp.arange(top)[None, :] + turn) % top, axis=1)


def portions_of(count, total, most, lean, full):
    portions = [(1 << 20) // math.isqrt(standing ** lean) + 1 for standing in range(1, count + 1)]
    largest = most if full else min(most, max(-(-total // count), total * portions[0] // sum(portions)))
    least = 1 if total - largest >= count - 1 else 0
    given, surplus = [largest] + [least] * (count - 1), total - largest - least * (count - 1)
    while surplus > 0:
        movable = [i for i in range(1, count) if given[i] < largest] or [i for i in range(1, count) if given[i] < most]
        whole, left = sum([portions[i] for i in movable]), surplus
        for i in movable:
            extra = min(most - given[i], max(1, left * portions[i] // whole), surplus)
            given[i] = given[i] + extra
            surplus = surplus - extra
    return np.array(given)


def gaussian(key, shape, spread, limit, pieces=(), kind=jnp.bfloat16):
    factor_of = steps_of(key, shape, pieces, -0.22, 0.18) if pieces else 1.0
    result = jax.random.normal(key, shape, jnp.float32) * spread * factor_of
    return jnp.minimum(jnp.maximum(result, -limit), limit).astype(kind)


def setup_inputs(seed: int = 0) -> dict:
    key_list = jax.random.split(jax.random.key(seed), 7)
    tokens = gaussian(key_list[0], (TOKENS, D), 1.0, 6.0, ((0, 16), (1, 16)))
    routes_keys = jax.random.split(jax.random.fold_in(key_list[1], 1), TOKENS // TOK_DEV)
    routes_turns = jax.random.permutation(jax.random.fold_in(key_list[1], 3), TOKENS // TOK_DEV)
    routes = jax.vmap(lambda own, number: deal_out(jax.random.fold_in(key_list[1], 2), own, number, TOK_DEV, EXPERTS, TOP, CAP, 2))(routes_keys, routes_turns).reshape((TOKENS, TOP))
    gates = jnp.clip(0.05 + 0.45 * jax.random.uniform(key_list[2], (TOKENS, TOP), jnp.float32) ** steps_of(key_list[2], (TOKENS, TOP), ((0, 16),), -0.2, 0.2), 0.05, 0.5)
    w_gate = gaussian(key_list[3], (EXPERTS, D, FF), D ** -0.5, 0.0625, ((0, 16), (2, 16)))
    w_up = gaussian(key_list[4], (EXPERTS, D, FF), D ** -0.5, 0.0625, ((0, 16), (2, 16)))
    w_down = gaussian(key_list[5], (EXPERTS, FF, D), FF ** -0.5, 0.125, ((0, 16), (1, 16)))
    return dict(tokens=tokens, routes=routes, gates=gates, w_gate=w_gate, w_up=w_up, w_down=w_down)


def reference(tokens, routes, gates, w_gate, w_up, w_down):
    grouped = routes.reshape(N_COL, TOK_DEV * TOP)
    onehot = (grouped[:, :, None] == jnp.arange(EXPERTS, dtype=jnp.int32)[None, None, :]).astype(jnp.int32)
    before = jnp.cumsum(onehot, axis=1) - onehot
    position = jnp.sum(before * onehot, axis=2).astype(jnp.int32)
    group_ids = jnp.arange(N_COL, dtype=jnp.int32)[:, None]
    destination = (grouped * SLOTS + group_ids * CAP + position).reshape(-1)
    source_rows = jnp.arange(TOKENS * TOP, dtype=jnp.int32) // TOP
    dispatched = jnp.zeros((EXPERTS * SLOTS, D), jnp.bfloat16).at[destination].set(tokens[source_rows])
    dispatched = dispatched.reshape(EXPERTS, SLOTS, D)

    def expert(operands):
        inputs, gate_matrix, up_matrix, down_matrix = operands
        gate_act = jnp.dot(inputs, gate_matrix, preferred_element_type=jnp.float32)
        up_act = jnp.dot(inputs, up_matrix, preferred_element_type=jnp.float32)
        hidden = (jax.nn.silu(gate_act) * up_act).astype(jnp.bfloat16)
        partial_value = jnp.einsum("rcf,cfd->crd", hidden.reshape(SLOTS, N_ROW, FF_BLOCK).astype(jnp.float32),
                             down_matrix.reshape(N_ROW, FF_BLOCK, D).astype(jnp.float32))
        rounded = lax.optimization_barrier(partial_value.astype(jnp.bfloat16))
        return jnp.sum(rounded.astype(jnp.float32), axis=0).astype(jnp.bfloat16)

    outputs = lax.map(expert, (dispatched, w_gate, w_up, w_down))
    picked = outputs.reshape(EXPERTS * SLOTS, D)[destination].reshape(TOKENS, TOP, D)
    mixed = jnp.sum(gates[:, :, None] * picked.astype(jnp.float32), axis=1)
    return mixed.astype(jnp.bfloat16)
```

```python
import functools

import jax
import jax.numpy as jnp
from jax import lax
from jax.experimental import pallas as pl
from jax.experimental.pallas import tpu as pltpu
from jax.sharding import Mesh
from jax.sharding import PartitionSpec as P


FEATS = 448
PAIR = 128
BLOCKS = 16
HALF = BLOCKS // 2
HELD = 2
UNITS = 128

ORDERS = (
    (("x", 0), ("x", 1), ("y", 0), ("y", 1)),
    (("x", 1), ("x", 0), ("y", 1), ("y", 0)),
    (("y", 0), ("y", 1), ("x", 0), ("x", 1)),
    (("y", 1), ("y", 0), ("x", 1), ("x", 0)),
)
COLOURS = len(ORDERS)


def partner(i, kind):
    if kind == 0:
        return i ^ 1
    return (i + 1) % 4 if i % 2 else (i - 1) % 4


def swap(value, axis, kind):
    return lax.ppermute(value, axis, [(i, partner(i, kind)) for i in range(4)])


def place(i, own, kind):
    near = own ^ 1
    far = (own + jnp.where(own % 2 == 1, 1, 3)) % 4
    first, second = (near, far) if kind == 0 else (far, near)
    return jnp.where(i == own, 0, jnp.where(i == first, 1, jnp.where(i == second, 2, 3)))


def position(colour, block, own_y, own_x):
    kind = colour % 2
    at_y = place(block // 4, own_y, kind)
    at_x = place(block % 4, own_x, kind)
    return at_y * 4 + at_x if colour < 2 else at_x * 4 + at_y


def up_body(part, own_ref, *refs):
    x_refs, w_refs = refs[:COLOURS], refs[COLOURS : COLOURS + 4]
    rest = refs[COLOURS + 4 :]
    step = pl.program_id(0)
    if part == 0:
        (acc_ref,) = rest
    else:
        start_ref, scale_ref, hidden_ref, acc_ref = rest

    @pl.when(step == 0)
    def _():
        if part == 0:
            acc_ref[...] = jnp.zeros_like(acc_ref)
        else:
            acc_ref[...] = start_ref[...]

    gate_refs, up_refs = (w_refs[0], w_refs[1]), (w_refs[2], w_refs[3])
    for colour in range(COLOURS):
        at = position(colour, step, own_ref[0], own_ref[1]) - part * HALF

        @pl.when(jnp.logical_and(at >= 0, at < HALF))
        def _(colour=colour, at=at):
            rows = x_refs[colour][pl.ds(pl.multiple_of(at * FEATS, FEATS), FEATS), :]
            rows = rows.T
            for e in range(2 * HELD):
                w = jnp.concatenate(
                    [gate_refs[e // HELD][e % HELD], up_refs[e // HELD][e % HELD]], axis=1
                )
                acc_ref[colour, :, e * 256 : (e + 1) * 256] += jnp.dot(
                    rows, w, preferred_element_type=jnp.float32
                )

    if part == 1:

        @pl.when(step == BLOCKS - 1)
        def _():
            for colour in range(COLOURS):
                for e in range(2 * HELD):
                    g = acc_ref[colour, :, e * 256 : e * 256 + UNITS]
                    u = acc_ref[colour, :, e * 256 + UNITS : (e + 1) * 256]
                    scale = scale_ref[colour * PAIR : (colour + 1) * PAIR, e : e + 1]
                    h = g / (1.0 + jnp.exp(-g)) * u * scale
                    hidden_ref[
                        colour * PAIR : (colour + 1) * PAIR, e * UNITS : (e + 1) * UNITS
                    ] = h.astype(jnp.bfloat16)


def up_part(part, own, xs, weights, start=None, scale=None):
    acc = jax.ShapeDtypeStruct((COLOURS, PAIR, 2 * HELD * 256), jnp.float32)
    whole = lambda shape: pl.BlockSpec(shape, lambda f, o: (0,) * len(shape))
    in_specs = [whole((HALF * FEATS, PAIR))] * COLOURS
    in_specs += [pl.BlockSpec((HELD, FEATS, UNITS), lambda f, o: (0, f, 0))] * 4
    args = list(xs) + list(weights)
    scratch = []
    if part == 0:
        out_shape, out_specs = acc, whole(acc.shape)
    else:
        in_specs += [whole(acc.shape), whole(scale.shape)]
        args += [start, scale]
        out_shape = jax.ShapeDtypeStruct((COLOURS * PAIR, 2 * HELD * UNITS), jnp.bfloat16)
        out_specs = whole(out_shape.shape)
        scratch = [pltpu.VMEM(acc.shape, jnp.float32)]
    return pl.pallas_call(
        functools.partial(up_body, part),
        out_shape=out_shape,
        grid_spec=pltpu.PrefetchScalarGridSpec(
            num_scalar_prefetch=1,
            grid=(BLOCKS,),
            in_specs=in_specs,
            out_specs=out_specs,
            scratch_shapes=scratch,
        ),
        cost_estimate=pl.CostEstimate(
            flops=3_800_000_000, bytes_accessed=20_000_000, transcendentals=0
        ),
        name=f"up{part}",
    )(own, *args)


def down_body(part, own_ref, hidden_ref, own_w_ref, other_w_ref, *out_refs):
    step = pl.program_id(0)
    w = jnp.concatenate(
        [own_w_ref[0], own_w_ref[1], other_w_ref[0], other_w_ref[1]], axis=0
    )
    for colour in range(COLOURS):
        at = [
            position(colour, 2 * step + i, own_ref[0], own_ref[1]) - part * HALF
            for i in range(2)
        ]
        inside = [jnp.logical_and(a >= 0, a < HALF) for a in at]

        @pl.when(jnp.logical_or(inside[0], inside[1]))
        def _(colour=colour, at=at, inside=inside):
            value = jnp.dot(
                hidden_ref[colour * PAIR : (colour + 1) * PAIR, :],
                w,
                preferred_element_type=jnp.float32,
            )
            value = value.astype(jnp.bfloat16).T
            for i in range(2):

                @pl.when(inside[i])
                def _(i=i):
                    out_refs[colour][pl.ds(pl.multiple_of(at[i] * FEATS, FEATS), FEATS), :] = (
                        value[i * FEATS : (i + 1) * FEATS]
                    )


def down_part(part, own, hidden, own_w, other_w):
    whole = lambda shape: pl.BlockSpec(shape, lambda q, o: (0,) * len(shape))
    out = jax.ShapeDtypeStruct((HALF * FEATS, PAIR), jnp.bfloat16)
    return pl.pallas_call(
        functools.partial(down_body, part),
        out_shape=[out] * COLOURS,
        grid_spec=pltpu.PrefetchScalarGridSpec(
            num_scalar_prefetch=1,
            grid=(BLOCKS // 2,),
            in_specs=[
                whole(hidden.shape),
                pl.BlockSpec((HELD, UNITS, 2 * FEATS), lambda q, o: (0, 0, q)),
                pl.BlockSpec((HELD, UNITS, 2 * FEATS), lambda q, o: (0, 0, q)),
            ],
            out_specs=[whole(out.shape)] * COLOURS,
        ),
        cost_estimate=pl.CostEstimate(
            flops=2_000_000_000, bytes_accessed=12_000_000, transcendentals=0
        ),
        name=f"down{part}",
    )(own, hidden, own_w, other_w)


def add(a, b):
    return (a.astype(jnp.float32) + b.astype(jnp.float32)).astype(jnp.bfloat16)


def shards(tokens, routes, gates, w_gate, w_up, w_down):
    own = jnp.stack([lax.axis_index("y"), lax.axis_index("x")]).astype(jnp.int32)
    z, core = lax.axis_index("z"), lax.axis_index("core")

    high = lax.reduce_precision(gates, 8, 7)
    middle = lax.reduce_precision(gates - high, 8, 7)
    low = gates - high - middle
    side = jnp.concatenate([routes.astype(jnp.float32), high, middle, low], axis=1)
    block = jnp.concatenate([tokens, side.astype(jnp.bfloat16)], axis=1).T
    near = lax.ppermute(block, "z", [(i, i ^ 1) for i in range(8)])
    pairs = [jnp.concatenate([block, near], axis=1)]
    for j in range(1, COLOURS):
        pairs.append(lax.ppermute(pairs[0], "z", [(i, (i - 2 * j) % 8) for i in range(8)]))

    other = [lax.ppermute(w, "core", [(0, 1), (1, 0)]) for w in (w_gate, w_up, w_down)]

    held = [p[:FEATS] for p in pairs]
    for step in range(3):
        got = [swap(held[c], *ORDERS[c][step]) for c in range(COLOURS)]
        held = [jnp.concatenate([h, g], axis=0) for h, g in zip(held, got)]
    last = [swap(held[c], *ORDERS[c][3]) for c in range(COLOURS)]

    sides = jnp.stack([p[FEATS:] for p in pairs]).astype(jnp.float32)
    named = sides[:, :8]
    weight = sides[:, 8:16] + sides[:, 16:24] + sides[:, 24:32]
    expert = (2 * (2 * z + core) + jnp.arange(2 * HELD)) % 4 + 4 * z
    scale = jnp.sum(
        jnp.where(named[:, None] == expert[None, :, None, None], weight[:, None], 0.0), axis=2
    )
    scale = scale.transpose(0, 2, 1).reshape(COLOURS * PAIR, 2 * HELD)

    weights = (w_gate, other[0], w_up, other[1])
    acc = up_part(0, own, held, weights)
    hidden = up_part(1, own, last, weights, acc, scale)
    away = down_part(1, own, hidden, w_down, other[2])
    kept = down_part(0, own, hidden, w_down, other[2])

    for step in (3, 2, 1, 0):
        got = [swap(away[c], *ORDERS[c][step]) for c in range(COLOURS)]
        kept = [add(k, g) for k, g in zip(kept, got)]
        if step:
            rows = kept[0].shape[0] // 2
            away = [k[rows:] for k in kept]
            kept = [k[:rows] for k in kept]

    total = kept[0].astype(jnp.float32)
    for j in range(1, COLOURS):
        got = lax.ppermute(kept[j], "z", [(i, (i + 2 * j) % 8) for i in range(8)])
        total = total + got.astype(jnp.float32)
    rows = PAIR // 2
    got = lax.ppermute(
        total[:, rows:].astype(jnp.bfloat16), "z", [(i, i ^ 1) for i in range(8)]
    )
    return (total[:, :rows] + got.astype(jnp.float32)).T.astype(jnp.bfloat16)


def solution(mesh):
    sizes = (4, 4, 8, 2)
    grid = Mesh(mesh.devices.reshape(sizes), ("y", "x", "z", "core"))
    row, col = ("y", "x"), ("z", "core")
    return jax.shard_map(
        shards,
        mesh=grid,
        in_specs=(
            P(col, row),
            P(col, None),
            P(col, None),
            P(col, None, row),
            P(col, None, row),
            P(col, row, None),
        ),
        out_specs=P(col, row),
        check_vma=False,
    )
```

```python
import functools

import jax
import jax.numpy as jnp
import numpy as np
from jax import lax
from jax.experimental import pallas as pl
from jax.experimental.pallas import tpu as pltpu
from jax.sharding import Mesh
from jax.sharding import PartitionSpec as P


FEATS = 448
PAIR = 128
BLOCKS = 16
QUARTER = BLOCKS // 4
HELD = 2
TOP = 8
TOKENS = 64
UNITS = 128
WIDE = 512

ORDERS = (
    (("x", 0), ("x", 1), ("y", 0), ("y", 1)),
    (("x", 1), ("x", 0), ("y", 1), ("y", 0)),
    (("y", 0), ("y", 1), ("x", 0), ("x", 1)),
    (("y", 1), ("y", 0), ("x", 1), ("x", 0)),
)
COLOURS = len(ORDERS)


def partner(i, kind, size):
    if kind == 0:
        return i ^ 1
    return (i + 1) % size if i % 2 else (i - 1) % size


def swap(value, axis, kind):
    size = lax.axis_size(axis)
    return lax.ppermute(value, axis, [(i, partner(i, kind, size)) for i in range(size)])


def ring_list(own, kind):
    first, second = partner(own, kind, 4), partner(own, 1 - kind, 4)
    return [own, first, second, partner(second, kind, 4)]


def block_table():
    table = np.zeros((4, 4, COLOURS, BLOCKS), np.int32)
    for y, x, colour, place in np.ndindex(*table.shape):
        ys, xs = ring_list(y, colour % 2), ring_list(x, colour % 2)
        outer, inner = place // 4, place % 4
        at_y, at_x = (outer, inner) if colour < 2 else (inner, outer)
        table[y, x, colour, place] = ys[at_y] * 4 + xs[at_x]
    return table.reshape(BLOCKS, COLOURS * BLOCKS)


def block_of(colour, place, own_ref):
    return own_ref[colour * BLOCKS + place]


def in_vmem(arrays):
    return [pltpu.with_memory_space_constraint(a, pltpu.VMEM) for a in arrays]


VMEM = pl.BlockSpec(memory_space=pltpu.VMEM)
SMEM = pl.BlockSpec(memory_space=pltpu.SMEM)


def call(body, name, out_shape, smem, arrays, flops, scratch=(), limit=12 << 20):
    return pl.pallas_call(
        body,
        out_shape=[pltpu.VMEM(*o) for o in out_shape],
        in_specs=[SMEM] * len(smem) + [VMEM] * len(arrays),
        out_specs=[VMEM] * len(out_shape),
        scratch_shapes=list(scratch),
        compiler_params=pltpu.CompilerParams(vmem_limit_bytes=limit),
        cost_estimate=pl.CostEstimate(flops=flops, bytes_accessed=1_000_000, transcendentals=0),
        name=name,
    )(*smem, *in_vmem(arrays))


def head_body(tokens_ref, routes_ref, gates_ref, out_ref):
    out_ref[:FEATS, :] = tokens_ref[...].astype(jnp.float32).T.astype(jnp.bfloat16)
    gates = gates_ref[...]
    high = gates.astype(jnp.bfloat16).astype(jnp.float32)
    middle = (gates - high).astype(jnp.bfloat16).astype(jnp.float32)
    low = gates - high - middle
    side = jnp.concatenate([routes_ref[...].astype(jnp.float32), high, middle, low], axis=0)
    out_ref[FEATS:, :] = side.astype(jnp.bfloat16)


def up_body(part, own_ref, *refs):
    x_refs, w_refs = refs[:COLOURS], refs[COLOURS : COLOURS + 4]
    rest = refs[COLOURS + 4 :]
    out_ref, turned_ref = rest[-2:]
    last = part == 3
    for colour in range(COLOURS):
        for place in range(QUARTER):
            turned_ref[colour, place] = x_refs[colour][place * FEATS : (place + 1) * FEATS, :].T

    for core in range(2):
        gate_ref, up_ref = w_refs[core], w_refs[2 + core]

        @pl.loop(0, HELD)
        def _(e, core=core, gate_ref=gate_ref, up_ref=up_ref):
            for colour in range(COLOURS):
                total = None
                for place in range(QUARTER):
                    block = block_of(colour, place + part * QUARTER, own_ref)
                    rows = pl.ds(pl.multiple_of(block * FEATS, FEATS), FEATS)
                    w = jnp.concatenate([gate_ref[e, rows, :], up_ref[e, rows, :]], axis=1)
                    value = jnp.dot(
                        turned_ref[colour, place], w, preferred_element_type=jnp.float32
                    )
                    total = value if total is None else total + value
                if part:
                    total = total + rest[0][core * HELD + e, colour]
                if last:
                    side = rest[1 + colour][FEATS:, :].astype(jnp.float32)
                    named = side[:TOP]
                    weight = side[TOP : 2 * TOP] + side[2 * TOP : 3 * TOP] + side[3 * TOP :]
                    g, u = total[:, :UNITS], total[:, UNITS:]
                    expert = (own_ref[COLOURS * BLOCKS + core] + e).astype(jnp.float32)
                    scale = jnp.sum(jnp.where(named == expert, weight, 0.0), axis=0, keepdims=True)
                    scale = jnp.broadcast_to(scale, (UNITS, PAIR)).T
                    total = (g / (1.0 + jnp.exp(-g)) * u * scale).astype(jnp.bfloat16)
                out_ref[core * HELD + e, colour] = total


def up_part(part, own, xs, weights, more):
    if part < 3:
        out = ((2 * HELD, COLOURS, PAIR, 2 * UNITS), jnp.float32)
    else:
        out = ((2 * HELD, COLOURS, PAIR, UNITS), jnp.bfloat16)
    return call(
        functools.partial(up_body, part),
        f"up{part}",
        [out],
        [own],
        [*xs, *weights, *more],
        2_000_000_000,
        [pltpu.VMEM((COLOURS, QUARTER, PAIR, FEATS), jnp.bfloat16)],
    )[0]


def widen_body(own_w_ref, other_w_ref, out_ref):
    for core, ref in enumerate((own_w_ref, other_w_ref)):
        for e in range(HELD):
            for block in range(BLOCKS):
                out_ref[core * HELD + e, :, block * WIDE : block * WIDE + FEATS] = ref[
                    e, :, block * FEATS : (block + 1) * FEATS
                ]


def down_body(part, colours, own_ref, hidden_ref, w_ref, *out_refs):
    for colour, out_ref in zip(colours, out_refs):
        hidden = jnp.concatenate([hidden_ref[e, colour] for e in range(2 * HELD)], axis=1)
        for place in range(QUARTER):
            block = block_of(colour, place + part * QUARTER, own_ref)
            columns = pl.ds(pl.multiple_of(block * WIDE, WIDE), FEATS)
            w = jnp.concatenate([w_ref[e, :, columns] for e in range(2 * HELD)], axis=0)
            value = jnp.dot(hidden, w, preferred_element_type=jnp.float32)
            out_ref[place * FEATS : (place + 1) * FEATS, :] = value.astype(jnp.bfloat16).T


def down_part(part, colours, own, hidden, w):
    return call(
        functools.partial(down_body, part, colours),
        f"down{part}_" + "".join(map(str, colours)),
        [((QUARTER * FEATS, PAIR), jnp.bfloat16)] * len(colours),
        [own],
        [hidden, w],
        250_000_000 * len(colours),
    )


def add(a, b):
    return (a.astype(jnp.float32) + b.astype(jnp.float32)).astype(jnp.bfloat16)


def shards(tokens, routes, gates, w_gate, w_up, w_down):
    z, core = lax.axis_index("z"), lax.axis_index("core")
    first = [HELD * (2 * z + core), HELD * (2 * z + 1 - core)]
    row = lax.axis_index("y") * 4 + lax.axis_index("x")
    blocks = lax.dynamic_index_in_dim(jnp.asarray(block_table()), row, keepdims=False)
    own = jnp.concatenate([blocks, jnp.stack(first).astype(jnp.int32)])

    block = call(
        head_body,
        "head",
        [((FEATS + 4 * TOP, TOKENS), jnp.bfloat16)],
        [],
        [tokens, routes.T, gates.T],
        1_000_000,
    )[0]
    pairs = [jnp.concatenate([block, swap(block, "z", 0)], axis=1)]
    for j in range(1, COLOURS):
        pairs.append(lax.ppermute(pairs[0], "z", [(i, (i - 2 * j) % 8) for i in range(8)]))

    other = [lax.ppermute(w, "core", [(0, 1), (1, 0)]) for w in (w_gate, w_up, w_down)]

    every = range(COLOURS)
    quarter = [p[:FEATS] for p in pairs]
    for step in range(2):
        got = [swap(quarter[c], *ORDERS[c][step]) for c in every]
        quarter = [jnp.concatenate([h, g], axis=0) for h, g in zip(quarter, got)]
    weights = (w_gate, other[0], w_up, other[1])
    first, second = quarter, [swap(quarter[c], *ORDERS[c][2]) for c in every]
    third = [swap(first[c], *ORDERS[c][3]) for c in every]
    acc = up_part(0, own, first, weights, [])
    w_wide = call(
        widen_body,
        "widen",
        [((2 * HELD, UNITS, BLOCKS * WIDE), jnp.bfloat16)],
        [],
        [w_down, other[2]],
        2_000_000_000,
    )[0]
    second = [lax.optimization_barrier((s, acc, w_wide))[0] for s in second]
    fourth = [swap(second[c], *ORDERS[c][3]) for c in every]
    acc = up_part(1, own, second, weights, [acc])
    acc = up_part(2, own, third, weights, [acc])
    hidden = up_part(3, own, fourth, weights, [acc, *pairs])

    away = [down_part(3, (c,), own, hidden, w_wide)[0] for c in every]
    hidden = lax.optimization_barrier((hidden, *away))[0]
    got = [swap(away[c], *ORDERS[c][3]) for c in every]
    away = down_part(2, tuple(every), own, hidden, w_wide)
    near = [swap(away[c], *ORDERS[c][3]) for c in every]
    kept = down_part(1, tuple(every), own, hidden, w_wide)
    away = [add(k, g) for k, g in zip(kept, got)]
    got = [swap(away[c], *ORDERS[c][2]) for c in every]
    kept = down_part(0, tuple(every), own, hidden, w_wide)
    kept = [
        sum(a.astype(jnp.float32) for a in parts).astype(jnp.bfloat16)
        for parts in zip(kept, near, got)
    ]
    for step in (1, 0):
        rows = kept[0].shape[0] // 2
        got = [swap(k[rows:], *ORDERS[c][step]) for c, k in enumerate(kept)]
        kept = [add(k[:rows], g) for k, g in zip(kept, got)]

    total = kept[0].astype(jnp.float32)
    for j in range(1, COLOURS):
        got = lax.ppermute(kept[j], "z", [(i, (i + 2 * j) % 8) for i in range(8)])
        total = total + got.astype(jnp.float32)
    total = total.astype(jnp.bfloat16)
    got = swap(total[:, TOKENS:], "z", 0)
    return add(total[:, :TOKENS], got).T


def solution(mesh):
    sizes = (4, 4, 8, 2)
    grid = Mesh(mesh.devices.reshape(sizes), ("y", "x", "z", "core"))
    row, col = ("y", "x"), ("z", "core")
    return jax.shard_map(
        shards,
        mesh=grid,
        in_specs=(
            P(col, row),
            P(col, None),
            P(col, None),
            P(col, None, row),
            P(col, None, row),
            P(col, row, None),
        ),
        out_specs=P(col, row),
        check_vma=False,
    )
```

```python
import functools

import jax
import jax.numpy as jnp
import numpy as np
from jax import lax
from jax.experimental import pallas as pl
from jax.experimental.pallas import tpu as pltpu
from jax.sharding import Mesh
from jax.sharding import PartitionSpec as P


FEATS = 448
PAIR = 128
BLOCKS = 16
QUARTER = BLOCKS // 4
FIRST = (0, 1, 3)
QUARTERS = (1, 2, 1)
HELD = 2
TOP = 8
TOKENS = 64
UNITS = 128
WIDE = 512

ORDERS = (
    (("x", 0), ("x", 1), ("y", 0), ("y", 1)),
    (("x", 1), ("x", 0), ("y", 1), ("y", 0)),
    (("y", 0), ("y", 1), ("x", 0), ("x", 1)),
    (("y", 1), ("y", 0), ("x", 1), ("x", 0)),
)
COLOURS = len(ORDERS)


def partner(i, kind, size):
    if kind == 0:
        return i ^ 1
    return (i + 1) % size if i % 2 else (i - 1) % size


def swap(value, axis, kind):
    size = lax.axis_size(axis)
    return lax.ppermute(value, axis, [(i, partner(i, kind, size)) for i in range(size)])


def ring_list(own, kind):
    first, second = partner(own, kind, 4), partner(own, 1 - kind, 4)
    return [own, first, second, partner(second, kind, 4)]


def block_table():
    table = np.zeros((4, 4, COLOURS, BLOCKS), np.int32)
    for y, x, colour, place in np.ndindex(*table.shape):
        ys, xs = ring_list(y, colour % 2), ring_list(x, colour % 2)
        outer, inner = place // 4, place % 4
        at_y, at_x = (outer, inner) if colour < 2 else (inner, outer)
        table[y, x, colour, place] = ys[at_y] * 4 + xs[at_x]
    return table.reshape(BLOCKS, COLOURS * BLOCKS)


def block_of(colour, place, own_ref):
    return own_ref[colour * BLOCKS + place]


def in_vmem(arrays):
    return [pltpu.with_memory_space_constraint(a, pltpu.VMEM) for a in arrays]


VMEM = pl.BlockSpec(memory_space=pltpu.VMEM)
SMEM = pl.BlockSpec(memory_space=pltpu.SMEM)


def call(body, name, out_shape, smem, arrays, flops, scratch=(), limit=12 << 20):
    return pl.pallas_call(
        body,
        out_shape=[pltpu.VMEM(*o) for o in out_shape],
        in_specs=[SMEM] * len(smem) + [VMEM] * len(arrays),
        out_specs=[VMEM] * len(out_shape),
        scratch_shapes=list(scratch),
        compiler_params=pltpu.CompilerParams(vmem_limit_bytes=limit),
        cost_estimate=pl.CostEstimate(flops=flops, bytes_accessed=1_000_000, transcendentals=0),
        name=name,
    )(*smem, *in_vmem(arrays))


def head_body(tokens_ref, routes_ref, gates_ref, out_ref):
    out_ref[:FEATS, :] = tokens_ref[...].astype(jnp.float32).T.astype(jnp.bfloat16)
    gates = gates_ref[...]
    high = gates.astype(jnp.bfloat16).astype(jnp.float32)
    middle = (gates - high).astype(jnp.bfloat16).astype(jnp.float32)
    low = gates - high - middle
    side = jnp.concatenate([routes_ref[...].astype(jnp.float32), high, middle, low], axis=0)
    out_ref[FEATS:, :] = side.astype(jnp.bfloat16)


def twin(place):
    return (place & 1) * 2 + (place >> 1)


def up_body(part, own_ref, *refs):
    count = QUARTERS[part] * QUARTER
    x_count = QUARTERS[part] * COLOURS
    x_refs, w_ref, rest = refs[:x_count], refs[x_count], refs[x_count + 1 :]
    out_ref, turned_ref = rest[-2:]
    @pl.loop(0, QUARTER)
    def _(at):
        rows = pl.ds(pl.multiple_of(at * FEATS, FEATS), FEATS)
        for n, x_ref in enumerate(x_refs):
            quarter, colour = n // COLOURS, n % COLOURS
            place = quarter * QUARTER + at
            if colour % 2:
                place = (quarter ^ (part == 1)) * QUARTER + twin(at)
            lanes = slice((colour % 2) * PAIR, (colour % 2 + 1) * PAIR)
            turned_ref[colour // 2, place, lanes, :] = x_ref[rows, :].T

    @pl.loop(0, 2 * HELD)
    def _(e):
        for duo in range(COLOURS // 2):
            total = None
            for place in range(count):
                block = block_of(2 * duo, place + FIRST[part] * QUARTER, own_ref)
                rows = pl.ds(pl.multiple_of(block * FEATS, FEATS), FEATS)
                value = jnp.dot(
                    turned_ref[duo, place], w_ref[e, rows, :], preferred_element_type=jnp.float32
                )
                total = value if total is None else total + value
            if part:
                total = total + rest[0][e, duo]
            if part == 2:
                scales = []
                for i in range(2):
                    side = rest[1 + 2 * duo + i][FEATS:, :].astype(jnp.float32)
                    named = side[:TOP]
                    weight = side[TOP : 2 * TOP] + side[2 * TOP : 3 * TOP] + side[3 * TOP :]
                    expert = own_ref[COLOURS * BLOCKS + e].astype(jnp.float32)
                    scale = jnp.where(named == expert, weight, 0.0)
                    scale = jnp.sum(scale, axis=0, keepdims=True)
                    scales.append(jnp.broadcast_to(scale, (UNITS, PAIR)).T)
                g, u = total[:, :UNITS], total[:, UNITS:]
                total = g / (1.0 + jnp.exp(-g)) * u * jnp.concatenate(scales, axis=0)
                total = total.astype(jnp.bfloat16)
            out_ref[e, duo] = total


def up_part(part, own, xs, weights, more):
    lead = (2 * HELD, COLOURS // 2, 2 * PAIR)
    out = (lead + (2 * UNITS,), jnp.float32) if part < 2 else (lead + (UNITS,), jnp.bfloat16)
    count = QUARTERS[part] * QUARTER
    return call(
        functools.partial(up_body, part),
        f"up{part}",
        [out],
        [own],
        [*xs, weights, *more],
        2_000_000_000 * QUARTERS[part],
        [pltpu.VMEM((COLOURS // 2, count, 2 * PAIR, FEATS), jnp.bfloat16)],
        16 << 20,
    )[0]


def prepare_body(*refs):
    sources, downs = refs[:4], refs[4:6]
    both_ref, wide_ref, down_ref, done = refs[6:]
    copies = []
    for core, source in enumerate(downs):
        to = down_ref.at[core * HELD : (core + 1) * HELD]
        copies.append(pltpu.make_async_copy(source, to, done.at[core]))
    for n, source in enumerate(sources):
        core, half = n % 2, n // 2
        for e in range(HELD):
            to = both_ref.at[core * HELD + e, :, half * UNITS : (half + 1) * UNITS]
            copies.append(pltpu.make_async_copy(source.at[e], to, done.at[len(copies)]))
    for copy in copies:
        copy.start()
    copies[0].wait()
    copies[1].wait()

    @pl.loop(0, 2 * HELD)
    def _(e):
        for block in range(BLOCKS):
            wide_ref[e, :, block * WIDE : block * WIDE + FEATS] = down_ref[
                e, :, block * FEATS : (block + 1) * FEATS
            ]

    for copy in copies[2:]:
        copy.wait()


def prepare(sources, downs):
    hbm = pl.BlockSpec(memory_space=pltpu.HBM)
    model = sources[0].shape[1]
    args = [pltpu.with_memory_space_constraint(a, pltpu.HBM) for a in (*sources, *downs)]
    return pl.pallas_call(
        prepare_body,
        out_shape=[
            pltpu.VMEM((2 * HELD, model, 2 * UNITS), jnp.bfloat16),
            pltpu.VMEM((2 * HELD, UNITS, BLOCKS * WIDE), jnp.bfloat16),
        ],
        in_specs=[hbm] * 6,
        out_specs=[VMEM] * 2,
        scratch_shapes=[
            pltpu.VMEM((2 * HELD, UNITS, model), jnp.bfloat16),
            pltpu.SemaphoreType.DMA((2 + 4 * HELD,)),
        ],
        compiler_params=pltpu.CompilerParams(vmem_limit_bytes=12 << 20),
        cost_estimate=pl.CostEstimate(
            flops=2_000_000_000, bytes_accessed=40_000_000, transcendentals=0
        ),
        name="prepare",
    )(*args)


def down_body(part, duos, own_ref, hidden_ref, w_ref, *out_refs):
    count = 2 * len(duos)

    def at_place(place):
        for n, duo in enumerate(duos):
            hidden = jnp.concatenate([hidden_ref[e, duo] for e in range(2 * HELD)], axis=1)
            for quarter in range(QUARTERS[part]):
                block = block_of(2 * duo, place + (FIRST[part] + quarter) * QUARTER, own_ref)
                columns = pl.ds(pl.multiple_of(block * WIDE, WIDE), FEATS)
                w = jnp.concatenate([w_ref[e, :, columns] for e in range(2 * HELD)], axis=0)
                value = jnp.dot(hidden, w, preferred_element_type=jnp.float32)
                value = value.astype(jnp.bfloat16)
                for i, (q, at) in enumerate(
                    ((quarter, place), (quarter ^ (part == 1), twin(place)))
                ):
                    rows = pl.ds(pl.multiple_of(at * FEATS, FEATS), FEATS)
                    out_refs[q * count + 2 * n + i][rows, :] = value[i * PAIR : (i + 1) * PAIR].T

    unroll = 2 if part == 2 else 1

    @pl.loop(0, QUARTER // unroll)
    def _(n):
        for i in range(unroll):
            at_place(n * unroll + i)


def down_part(part, duos, own, hidden, w):
    count = 2 * len(duos) * QUARTERS[part]
    return call(
        functools.partial(down_body, part, duos),
        f"down{part}_" + "".join(map(str, duos)),
        [((QUARTER * FEATS, PAIR), jnp.bfloat16)] * count,
        [own],
        [hidden, w],
        250_000_000 * count,
    )


def add(a, b):
    return (a.astype(jnp.float32) + b.astype(jnp.float32)).astype(jnp.bfloat16)


def shards(tokens, routes, gates, w_gate, w_up, w_down):
    z, core = lax.axis_index("z"), lax.axis_index("core")
    experts = [HELD * (2 * z + c) + e for c in (core, 1 - core) for e in range(HELD)]
    row = lax.axis_index("y") * 4 + lax.axis_index("x")
    blocks = lax.dynamic_index_in_dim(jnp.asarray(block_table()), row, keepdims=False)
    own = jnp.concatenate([blocks, jnp.stack(experts).astype(jnp.int32)])

    block = call(
        head_body,
        "head",
        [((FEATS + 4 * TOP, TOKENS), jnp.bfloat16)],
        [],
        [tokens, routes.T, gates.T],
        1_000_000,
    )[0]
    pairs = [jnp.concatenate([block, swap(block, "z", 0)], axis=1)]
    for j in range(1, COLOURS):
        pairs.append(lax.ppermute(pairs[0], "z", [(i, (i - 2 * j) % 8) for i in range(8)]))

    other = [lax.ppermute(w, "core", [(0, 1), (1, 0)]) for w in (w_gate, w_up, w_down)]

    every = range(COLOURS)
    quarter = [p[:FEATS] for p in pairs]
    for step in range(2):
        got = [swap(quarter[c], *ORDERS[c][step]) for c in every]
        quarter = [jnp.concatenate([h, g], axis=0) for h, g in zip(quarter, got)]
    weights, w_wide = prepare((w_gate, other[0], w_up, other[1]), (w_down, other[2]))
    first, second = quarter, [swap(quarter[c], *ORDERS[c][2]) for c in every]
    third = [swap(first[c], *ORDERS[c][3]) for c in every]
    acc = up_part(0, own, first, weights, [])
    second = [lax.optimization_barrier((s, acc, w_wide))[0] for s in second]
    fourth = [swap(second[c], *ORDERS[c][3]) for c in every]
    acc = up_part(1, own, [*second, *third], weights, [acc])
    hidden = up_part(2, own, fourth, weights, [acc, *pairs])

    away = [*down_part(2, (0,), own, hidden, w_wide), *down_part(2, (1,), own, hidden, w_wide)]
    hidden = lax.optimization_barrier((hidden, *away))[0]
    got = [swap(away[c], *ORDERS[c][3]) for c in every]
    middle = down_part(1, (0, 1), own, hidden, w_wide)
    kept, away = middle[:COLOURS], middle[COLOURS:]
    near = [swap(away[c], *ORDERS[c][3]) for c in every]
    away = [add(k, g) for k, g in zip(kept, got)]
    got = [swap(away[c], *ORDERS[c][2]) for c in every]
    kept = down_part(0, (0, 1), own, hidden, w_wide)
    kept = [
        sum(a.astype(jnp.float32) for a in parts).astype(jnp.bfloat16)
        for parts in zip(kept, near, got)
    ]
    for step in (1, 0):
        rows = kept[0].shape[0] // 2
        got = [swap(k[rows:], *ORDERS[c][step]) for c, k in enumerate(kept)]
        kept = [add(k[:rows], g) for k, g in zip(kept, got)]

    total = kept[0].astype(jnp.float32)
    for j in range(1, COLOURS):
        got = lax.ppermute(kept[j], "z", [(i, (i + 2 * j) % 8) for i in range(8)])
        total = total + got.astype(jnp.float32)
    total = total.astype(jnp.bfloat16)
    got = swap(total[:, TOKENS:], "z", 0)
    return add(total[:, :TOKENS], got).T


def solution(mesh):
    sizes = (4, 4, 8, 2)
    grid = Mesh(mesh.devices.reshape(sizes), ("y", "x", "z", "core"))
    row, col = ("y", "x"), ("z", "core")
    return jax.shard_map(
        shards,
        mesh=grid,
        in_specs=(
            P(col, row),
            P(col, None),
            P(col, None),
            P(col, None, row),
            P(col, None, row),
            P(col, row, None),
        ),
        out_specs=P(col, row),
        check_vma=False,
    )
```

```python
import functools

import jax
import jax.numpy as jnp
import numpy as np
from jax import lax
from jax.experimental import pallas as pl
from jax.experimental.pallas import tpu as pltpu
from jax.sharding import Mesh
from jax.sharding import PartitionSpec as P


FEATS = 448
PAIR = 128
BLOCKS = 16
QUARTER = BLOCKS // 4
FIRST = (0, 1, 3)
QUARTERS = (1, 2, 1)
HELD = 2
TOP = 8
TOKENS = 64
UNITS = 128
WIDE = 512

ORDERS = (
    (("x", 0), ("x", 1), ("y", 0), ("y", 1)),
    (("x", 1), ("x", 0), ("y", 1), ("y", 0)),
    (("y", 0), ("y", 1), ("x", 0), ("x", 1)),
    (("y", 1), ("y", 0), ("x", 1), ("x", 0)),
)
COLOURS = len(ORDERS)


def partner(i, kind, size):
    if kind == 0:
        return i ^ 1
    return (i + 1) % size if i % 2 else (i - 1) % size


def swap(value, axis, kind):
    size = lax.axis_size(axis)
    return lax.ppermute(value, axis, [(i, partner(i, kind, size)) for i in range(size)])


def ring_list(own, kind):
    first, second = partner(own, kind, 4), partner(own, 1 - kind, 4)
    return [own, first, second, partner(second, kind, 4)]


def block_table():
    table = np.zeros((4, 4, COLOURS, BLOCKS), np.int32)
    for y, x, colour, place in np.ndindex(*table.shape):
        ys, xs = ring_list(y, colour % 2), ring_list(x, colour % 2)
        outer, inner = place // 4, place % 4
        at_y, at_x = (outer, inner) if colour < 2 else (inner, outer)
        table[y, x, colour, place] = ys[at_y] * 4 + xs[at_x]
    return table.reshape(BLOCKS, COLOURS * BLOCKS)


def block_of(colour, place, own_ref):
    return own_ref[colour * BLOCKS + place]


def in_vmem(arrays):
    return [pltpu.with_memory_space_constraint(a, pltpu.VMEM) for a in arrays]


VMEM = pl.BlockSpec(memory_space=pltpu.VMEM)
SMEM = pl.BlockSpec(memory_space=pltpu.SMEM)


def call(body, name, out_shape, smem, arrays, flops, scratch=(), limit=12 << 20):
    return pl.pallas_call(
        body,
        out_shape=[pltpu.VMEM(*o) for o in out_shape],
        in_specs=[SMEM] * len(smem) + [VMEM] * len(arrays),
        out_specs=[VMEM] * len(out_shape),
        scratch_shapes=list(scratch),
        compiler_params=pltpu.CompilerParams(vmem_limit_bytes=limit),
        cost_estimate=pl.CostEstimate(flops=flops, bytes_accessed=1_000_000, transcendentals=0),
        name=name,
    )(*smem, *in_vmem(arrays))


def head_body(tokens_hbm, routes_hbm, gates_hbm, out_ref, tokens_ref, routes_ref, gates_ref, done):
    copies = [
        pltpu.make_async_copy(tokens_hbm, tokens_ref, done.at[0]),
        pltpu.make_async_copy(routes_hbm, routes_ref, done.at[1]),
        pltpu.make_async_copy(gates_hbm, gates_ref, done.at[2]),
    ]
    for copy in copies:
        copy.start()
    for copy in copies:
        copy.wait()
    out_ref[:FEATS, :] = tokens_ref[...].astype(jnp.float32).T.astype(jnp.bfloat16)
    gates = gates_ref[...]
    high = gates.astype(jnp.bfloat16).astype(jnp.float32)
    middle = (gates - high).astype(jnp.bfloat16).astype(jnp.float32)
    low = gates - high - middle
    side = jnp.concatenate([routes_ref[...].astype(jnp.float32), high, middle, low], axis=0)
    out_ref[FEATS:, :] = side.astype(jnp.bfloat16)


def head(*arrays):
    args = [pltpu.with_memory_space_constraint(a, pltpu.HBM) for a in arrays]
    return pl.pallas_call(
        head_body,
        out_shape=pltpu.VMEM((FEATS + 4 * TOP, TOKENS), jnp.bfloat16),
        in_specs=[pl.BlockSpec(memory_space=pltpu.HBM)] * 3,
        out_specs=VMEM,
        scratch_shapes=[pltpu.VMEM(a.shape, a.dtype) for a in arrays]
        + [pltpu.SemaphoreType.DMA((3,))],
        compiler_params=pltpu.CompilerParams(vmem_limit_bytes=2 << 20),
        name="head",
    )(*args)


def twin(place):
    return (place & 1) * 2 + (place >> 1)


def up_body(part, own_ref, *refs):
    count = QUARTERS[part] * QUARTER
    x_count = QUARTERS[part] * COLOURS
    x_refs, w_ref, rest = refs[:x_count], refs[x_count], refs[x_count + 1 :]
    out_ref, turned_ref = rest[-2:]
    @pl.loop(0, QUARTER)
    def _(at):
        rows = pl.ds(pl.multiple_of(at * FEATS, FEATS), FEATS)
        for n, x_ref in enumerate(x_refs):
            quarter, colour = n // COLOURS, n % COLOURS
            place = quarter * QUARTER + at
            if colour % 2:
                place = (quarter ^ (part == 1)) * QUARTER + twin(at)
            lanes = slice((colour % 2) * PAIR, (colour % 2 + 1) * PAIR)
            turned_ref[colour // 2, place, lanes, :] = x_ref[rows, :].T

    @pl.loop(0, 2 * HELD)
    def _(e):
        for duo in range(COLOURS // 2):
            total = None
            for place in range(count):
                block = block_of(2 * duo, place + FIRST[part] * QUARTER, own_ref)
                rows = pl.ds(pl.multiple_of(block * FEATS, FEATS), FEATS)
                value = jnp.dot(
                    turned_ref[duo, place], w_ref[e, rows, :], preferred_element_type=jnp.float32
                )
                total = value if total is None else total + value
            if part:
                total = total + rest[0][e, duo]
            if part == 2:
                scales = []
                for i in range(2):
                    side = rest[1 + 2 * duo + i][FEATS:, :].astype(jnp.float32)
                    named = side[:TOP]
                    weight = side[TOP : 2 * TOP] + side[2 * TOP : 3 * TOP] + side[3 * TOP :]
                    expert = own_ref[COLOURS * BLOCKS + e].astype(jnp.float32)
                    scale = jnp.where(named == expert, weight, 0.0)
                    scale = jnp.sum(scale, axis=0, keepdims=True)
                    scales.append(jnp.broadcast_to(scale, (UNITS, PAIR)).T)
                g, u = total[:, :UNITS], total[:, UNITS:]
                total = g / (1.0 + jnp.exp(-g)) * u * jnp.concatenate(scales, axis=0)
                total = total.astype(jnp.bfloat16)
            out_ref[e, duo] = total


def up_part(part, own, xs, weights, more):
    lead = (2 * HELD, COLOURS // 2, 2 * PAIR)
    out = (lead + (2 * UNITS,), jnp.float32) if part < 2 else (lead + (UNITS,), jnp.bfloat16)
    count = QUARTERS[part] * QUARTER
    return call(
        functools.partial(up_body, part),
        f"up{part}",
        [out],
        [own],
        [*xs, weights, *more],
        2_000_000_000 * QUARTERS[part],
        [pltpu.VMEM((COLOURS // 2, count, 2 * PAIR, FEATS), jnp.bfloat16)],
        16 << 20,
    )[0]


def prepare_body(*refs):
    sources, downs = refs[:4], refs[4:6]
    both_ref, wide_ref, down_ref, done = refs[6:]
    copies = []
    for core, source in enumerate(downs):
        to = down_ref.at[core * HELD : (core + 1) * HELD]
        copies.append(pltpu.make_async_copy(source, to, done.at[core]))
    for n, source in enumerate(sources):
        core, half = n % 2, n // 2
        for e in range(HELD):
            to = both_ref.at[core * HELD + e, :, half * UNITS : (half + 1) * UNITS]
            copies.append(pltpu.make_async_copy(source.at[e], to, done.at[len(copies)]))
    for copy in copies:
        copy.start()
    copies[0].wait()
    copies[1].wait()

    @pl.loop(0, 2 * HELD)
    def _(e):
        for block in range(BLOCKS):
            wide_ref[e, :, block * WIDE : block * WIDE + FEATS] = down_ref[
                e, :, block * FEATS : (block + 1) * FEATS
            ]

    for copy in copies[2:]:
        copy.wait()


def prepare(sources, downs):
    hbm = pl.BlockSpec(memory_space=pltpu.HBM)
    model = sources[0].shape[1]
    args = [pltpu.with_memory_space_constraint(a, pltpu.HBM) for a in (*sources, *downs)]
    return pl.pallas_call(
        prepare_body,
        out_shape=[
            pltpu.VMEM((2 * HELD, model, 2 * UNITS), jnp.bfloat16),
            pltpu.VMEM((2 * HELD, UNITS, BLOCKS * WIDE), jnp.bfloat16),
        ],
        in_specs=[hbm] * 6,
        out_specs=[VMEM] * 2,
        scratch_shapes=[
            pltpu.VMEM((2 * HELD, UNITS, model), jnp.bfloat16),
            pltpu.SemaphoreType.DMA((2 + 4 * HELD,)),
        ],
        compiler_params=pltpu.CompilerParams(vmem_limit_bytes=12 << 20),
        cost_estimate=pl.CostEstimate(
            flops=2_000_000_000, bytes_accessed=40_000_000, transcendentals=0
        ),
        name="prepare",
    )(*args)


def down_body(part, duos, own_ref, hidden_ref, w_ref, *out_refs):
    count = 2 * len(duos)

    def at_place(place):
        for n, duo in enumerate(duos):
            hidden = jnp.concatenate([hidden_ref[e, duo] for e in range(2 * HELD)], axis=1)
            for quarter in range(QUARTERS[part]):
                block = block_of(2 * duo, place + (FIRST[part] + quarter) * QUARTER, own_ref)
                columns = pl.ds(pl.multiple_of(block * WIDE, WIDE), FEATS)
                w = jnp.concatenate([w_ref[e, :, columns] for e in range(2 * HELD)], axis=0)
                value = jnp.dot(hidden, w, preferred_element_type=jnp.float32)
                value = value.astype(jnp.bfloat16)
                for i, (q, at) in enumerate(
                    ((quarter, place), (quarter ^ (part == 1), twin(place)))
                ):
                    rows = pl.ds(pl.multiple_of(at * FEATS, FEATS), FEATS)
                    out_refs[q * count + 2 * n + i][rows, :] = value[i * PAIR : (i + 1) * PAIR].T

    unroll = 2 if part == 2 else 1

    @pl.loop(0, QUARTER // unroll)
    def _(n):
        for i in range(unroll):
            at_place(n * unroll + i)


def down_part(part, duos, own, hidden, w):
    count = 2 * len(duos) * QUARTERS[part]
    return call(
        functools.partial(down_body, part, duos),
        f"down{part}_" + "".join(map(str, duos)),
        [((QUARTER * FEATS, PAIR), jnp.bfloat16)] * count,
        [own],
        [hidden, w],
        250_000_000 * count,
    )


def add(a, b):
    return (a.astype(jnp.float32) + b.astype(jnp.float32)).astype(jnp.bfloat16)


def shards(tokens, routes, gates, w_gate, w_up, w_down):
    z, core = lax.axis_index("z"), lax.axis_index("core")
    experts = [HELD * (2 * z + c) + e for c in (core, 1 - core) for e in range(HELD)]
    row = lax.axis_index("y") * 4 + lax.axis_index("x")
    blocks = lax.dynamic_index_in_dim(jnp.asarray(block_table()), row, keepdims=False)
    own = jnp.concatenate([blocks, jnp.stack(experts).astype(jnp.int32)])

    block = head(tokens, routes.T, gates.T)
    pairs = [jnp.concatenate([block, swap(block, "z", 0)], axis=1)]
    for j in range(1, COLOURS):
        pairs.append(lax.ppermute(pairs[0], "z", [(i, (i - 2 * j) % 8) for i in range(8)]))

    other = [lax.ppermute(w, "core", [(0, 1), (1, 0)]) for w in (w_gate, w_up, w_down)]

    every = range(COLOURS)
    quarter = [p[:FEATS] for p in pairs]
    for step in range(2):
        got = [swap(quarter[c], *ORDERS[c][step]) for c in every]
        quarter = [jnp.concatenate([h, g], axis=0) for h, g in zip(quarter, got)]
    weights, w_wide = prepare((w_gate, other[0], w_up, other[1]), (w_down, other[2]))
    first, second = quarter, [swap(quarter[c], *ORDERS[c][2]) for c in every]
    third = [swap(first[c], *ORDERS[c][3]) for c in every]
    acc = up_part(0, own, first, weights, [])
    second = [lax.optimization_barrier((s, acc, w_wide))[0] for s in second]
    fourth = [swap(second[c], *ORDERS[c][3]) for c in every]
    acc = up_part(1, own, [*second, *third], weights, [acc])
    hidden = up_part(2, own, fourth, weights, [acc, *pairs])

    away = [*down_part(2, (0,), own, hidden, w_wide), *down_part(2, (1,), own, hidden, w_wide)]
    hidden = lax.optimization_barrier((hidden, *away))[0]
    got = [swap(away[c], *ORDERS[c][3]) for c in every]
    middle = down_part(1, (0, 1), own, hidden, w_wide)
    kept, away = middle[:COLOURS], middle[COLOURS:]
    near = [swap(away[c], *ORDERS[c][3]) for c in every]
    away = [add(k, g) for k, g in zip(kept, got)]
    got = [swap(away[c], *ORDERS[c][2]) for c in every]
    kept = down_part(0, (0, 1), own, hidden, w_wide)
    kept = [
        sum(a.astype(jnp.float32) for a in parts).astype(jnp.bfloat16)
        for parts in zip(kept, near, got)
    ]
    for step in (1, 0):
        rows = kept[0].shape[0] // 2
        got = [swap(k[rows:], *ORDERS[c][step]) for c, k in enumerate(kept)]
        kept = [add(k[:rows], g) for k, g in zip(kept, got)]

    total = kept[0].astype(jnp.float32)
    for j in range(1, COLOURS):
        got = lax.ppermute(kept[j], "z", [(i, (i + 2 * j) % 8) for i in range(8)])
        total = total + got.astype(jnp.float32)
    total = total.astype(jnp.bfloat16)
    got = swap(total[:, TOKENS:], "z", 0)
    return add(total[:, :TOKENS], got).T


def solution(mesh):
    sizes = (4, 4, 8, 2)
    grid = Mesh(mesh.devices.reshape(sizes), ("y", "x", "z", "core"))
    row, col = ("y", "x"), ("z", "core")
    return jax.shard_map(
        shards,
        mesh=grid,
        in_specs=(
            P(col, row),
            P(col, None),
            P(col, None),
            P(col, None, row),
            P(col, None, row),
            P(col, row, None),
        ),
        out_specs=P(col, row),
        check_vma=False,
    )
```
